32 devices in a mesh: centre: 4 (over y, core), sample: 8 (over z, x).
Axes of the slice: x: 2, y: 2, z: 4, core: 2. Of those that a mesh axis runs over, the one named last changes fastest.
Arguments:
- centres: bfloat16 [1024, 8192], P(None, 'centre'), may hold values from -40 to 40
- pool: bfloat16 [1024, 8192], P('centre', 'sample'), may hold values from -40 to 40
- labels: int32 [8192], P('sample'), may hold values from 0 to 143
- picks: int32 [2, 4096], P(None, 'sample'), may hold values from 0 to 8191, as said below
- coefs: float32 [144, 8192], P(None, ('centre', 'sample')), may hold values from -192 to 256000
Outputs:
- new_coefs: float32 [144, 8192], P(None, ('centre', 'sample'))
The draws below stay inside these ranges and needn't reach their ends.
Inputs may be any that keep to these rules, and one draw needn't show every extreme that they name: `picks`: entry b of a step's batch is a pool column in [(b // 512) * 1024, (b // 512 + 1) * 1024); entries may repeat.
All inputs are finite; a program needn't handle non-finite values.
Results may differ from the reference program's by a relative error of at most 0.00065.
Values may be sent and summed in bfloat16 or wider, within the bound.
A program may use at most 64 MiB of HBM per device.

```python
import jax
import jax.numpy as jnp
from jax import lax

D = 1024
K = 144
STEPS = 2
BATCH_DEV = 512
POOL_DEV = 1024
CENTRES = 8192
BATCH = 4096
POOL = 8192
N_SAMPLE = 8


GROUP_SHARED = 0.05


GROUP_NOISE = 0.15


GROUP_LEVEL = 128.0


WAVE_AMPLITUDE = 2.5


WAVE_RATE = 0.35


def column_scales(key, count, lower, upper):
    return jnp.exp(jax.random.uniform(key, (count,), jnp.float32, jnp.log(lower), jnp.log(upper)))


def latent_map(key):
    return jax.random.truncated_normal(jax.random.fold_in(key, 5001), -4.0, 4.0, (D, 8), jnp.float32)


def centre_latents(key):
    return jax.random.truncated_normal(jax.random.fold_in(key, 5002), -4.0, 4.0, (8, CENTRES), jnp.float32)


def pool_latents(key):
    return jax.random.truncated_normal(jax.random.fold_in(key, 5003), -4.0, 4.0, (8, POOL), jnp.float32)


def prototypes(key):
    return jax.random.truncated_normal(jax.random.fold_in(key, 6001), -4.0, 4.0, (D, 2 * K), jnp.float32)


def centre_groups(key):
    return jax.random.randint(jax.random.fold_in(key, 6003), (CENTRES,), 0, 2 * K, jnp.int32)


def pool_groups(key):
    return jax.random.randint(jax.random.fold_in(key, 6004), (POOL,), 0, 2 * K, jnp.int32)


def grouped_columns(key, groups, latents, salt, lower, upper):
    scales = column_scales(jax.random.fold_in(key, 6002), 2 * K, lower, upper)
    base = jnp.take(prototypes(key), groups, axis=1)
    jitter = jax.random.truncated_normal(jax.random.fold_in(key, salt), -4.0, 4.0, (D, groups.shape[0]), jnp.float32)
    shared = jnp.dot(latent_map(key), latents, precision=lax.Precision.HIGHEST)
    return jnp.take(scales, groups)[None, :] * (base + GROUP_SHARED * shared + GROUP_NOISE * jitter)


def draw_centres(key, part):
    groups = centre_groups(key)
    columns = grouped_columns(key, groups, centre_latents(key), 11, 0.5, 2.0)
    return jnp.clip(columns, -40.0, 40.0).astype(jnp.bfloat16)


def draw_pool(key, part):
    groups = pool_groups(key)
    columns = grouped_columns(key, groups, pool_latents(key), 13, 0.5, 2.0)
    return jnp.clip(columns, -40.0, 40.0).astype(jnp.bfloat16)


def draw_picks(key, part):
    offsets = jax.random.randint(jax.random.fold_in(key, 31), (STEPS, BATCH), 0, POOL_DEV, jnp.int32)
    starts = jnp.arange(BATCH, dtype=jnp.int32) // BATCH_DEV * POOL_DEV
    return offsets + starts[None, :]


def draw_coefs(key, part):
    frequency = WAVE_RATE * jax.random.normal(jax.random.fold_in(key, 41), (256, 8), jnp.float32)
    phases = jax.random.uniform(jax.random.fold_in(key, 42), (256, 1), jnp.float32, -3.14159265, 3.14159265)
    wave_table = jnp.cos(jnp.dot(frequency, centre_latents(key), precision=lax.Precision.HIGHEST) + phases)
    groups = centre_groups(key)
    mixing = jax.random.uniform(jax.random.fold_in(key, 43), (K, 256), jnp.float32, -1.0, 1.0)
    jitter = jax.random.uniform(jax.random.fold_in(key, 22), (K, CENTRES), jnp.float32, -0.3, 0.3)
    group_table = GROUP_LEVEL * jax.random.uniform(jax.random.fold_in(key, 44), (K, 2 * K), jnp.float32, -1.0, 1.0)
    columns = WAVE_AMPLITUDE / 16.0 * jnp.dot(mixing, wave_table, precision=lax.Precision.HIGHEST) + jitter
    columns = columns + jnp.take(group_table, groups, axis=1)
    return columns.astype(jnp.float32)


def touch_ends(result, own_key, smallest, high):
    spot = [jax.random.randint(jax.random.fold_in(own_key, axis), (), 0, length) for axis, length in enumerate(result.shape)]
    widest = result.shape.index(max(result.shape))
    next_to = spot[:widest] + [(spot[widest] + 1) % result.shape[widest]] + spot[widest + 1:]
    return result.at[tuple(spot)].set(smallest).at[tuple(next_to)].set(high)


def setup_inputs(seed: int = 0) -> dict:
    streams_of = jax.random.split(jax.random.key(seed), 6)
    centres = draw_centres(jax.random.fold_in(streams_of[5], 71), 0)
    pool = draw_pool(jax.random.fold_in(streams_of[5], 71), 0)
    labels = touch_ends(jax.random.randint(streams_of[2], (POOL,), 0, K), jax.random.fold_in(streams_of[2], 1), 0, K - 1).astype(jnp.int32)
    picks = draw_picks(jax.random.fold_in(streams_of[5], 71), 0)
    coefs = draw_coefs(jax.random.fold_in(streams_of[5], 71), 0)
    return dict(centres=centres, pool=pool, labels=labels, picks=picks, coefs=coefs)


LOGIT_GAIN = 16.0
LENGTH_SCALE = 0.5
STEP_GAIN = 2048.0
EPS = 1e-06

def laplace(cross, sample_sq, centre_sq):
    mean_sq = (sample_sq[:, None] + centre_sq[None, :] - 2.0 * cross) / D
    return jnp.exp(-jnp.sqrt(mean_sq + EPS) / LENGTH_SCALE).astype(jnp.bfloat16)

def residual(logits, labs):
    classes = jnp.arange(K, dtype=jnp.int32)
    top = lax.optimization_barrier(jnp.max(logits, axis=0, keepdims=True))
    expo = jnp.exp(logits - top)
    probs = expo / lax.optimization_barrier(jnp.sum(expo, axis=0, keepdims=True))
    hot = (classes[:, None] == labs[None, :]).astype(jnp.float32)
    return (probs - hot).astype(jnp.bfloat16)

def reference(centres, pool, labels, picks, coefs):
    centre_sq = lax.optimization_barrier(jnp.sum(jnp.square(centres.astype(jnp.float32)), axis=0))
    for step in range(STEPS):
        blocks = picks[step].reshape(N_SAMPLE, BATCH_DEV)
        coef_half = coefs.astype(jnp.bfloat16)

        def visit(total, block):
            feats = jnp.take(pool, block, axis=1)
            cross = lax.dot_general(feats, centres, (((0,), (0,)), ((), ())), preferred_element_type=jnp.float32)
            sample_sq = lax.optimization_barrier(jnp.sum(jnp.square(feats.astype(jnp.float32)), axis=0))
            kern = laplace(cross, sample_sq, centre_sq)
            logits = lax.dot_general(coef_half, kern, (((1,), (1,)), ((), ())), preferred_element_type=jnp.float32)
            logits = logits * (LOGIT_GAIN / CENTRES)
            resid = residual(logits, jnp.take(labels, block))
            return (total + jnp.dot(resid, kern, preferred_element_type=jnp.float32), None)
        grad, _ = lax.scan(visit, jnp.zeros((K, CENTRES), jnp.float32), blocks)
        coefs = coefs - STEP_GAIN * LOGIT_GAIN / BATCH * grad
    return coefs
```

```python
import functools
import math

import jax
import jax.numpy as jnp
from jax import lax
from jax.experimental import pallas as pl
from jax.experimental.pallas import tpu as pltpu
from jax.sharding import PartitionSpec as P

LOGIT_GAIN = 16.0
LENGTH_SCALE = 0.5
STEP_GAIN = 2048.0
EPS = 1e-06

GRAD_WIRE = jnp.float32
LOGIT_WIRE = jnp.float32
MESH = pl.DeviceIdType.MESH
NT = (((1,), (1,)), ((), ()))


def kernel(
    n_c, n_s, logit_scale, rate,
    cen_hbm, pool_ref, labels_ref, picks_ref, coefs_ref, out_ref,
    cen, csq, feats, kern, labs, coefb, lsend, lrecv, resid, gsend, grecv, cur,
    cen_sem, send_sem, feat_sem, log_sem, res_sem, coef_sem, grad_sem,
):
    steps, batch = picks_ref.shape
    fd, pool_dev = pool_ref.shape
    classes, own = coefs_ref.shape
    width, cen_dev = cen.shape
    share = batch // n_c
    ny = n_c // 2
    tile = max(own, min(256, cen_dev))
    pieces = tile // own

    c = lax.axis_index("centre")
    s = lax.axis_index("sample")
    sib = c + 1 - 2 * lax.rem(c, 2)
    c_peers = [lax.rem(c + r, n_c) for r in range(1, n_c)]
    s_peers = [lax.rem(s + r, n_s) for r in range(1, n_s)]

    barrier = pltpu.get_barrier_semaphore()
    for peer in c_peers:
        pl.semaphore_signal(barrier, inc=1, device_id={"centre": peer}, device_id_type=MESH)
    for peer in s_peers:
        pl.semaphore_signal(barrier, inc=1, device_id={"sample": peer}, device_id_type=MESH)

    load = pltpu.make_async_copy(cen_hbm, cen, cen_sem)
    load.start()
    started = []

    def send(src, dst, recv, axis, peer):
        copy = pltpu.make_async_remote_copy(
            src_ref=src, dst_ref=dst, send_sem=send_sem.at[len(started)], recv_sem=recv,
            device_id={axis: peer}, device_id_type=MESH,
        )
        copy.start()
        started.append(copy)
        return copy

    label_rows = jnp.broadcast_to(labels_ref[...].astype(jnp.float32), (16, pool_dev)).astype(jnp.bfloat16)

    def pick(t):
        chosen = picks_ref[t:t + 1, :] - s * pool_dev
        rows = lax.broadcasted_iota(jnp.int32, (pool_dev, batch), 0)
        hot = jnp.where(rows == chosen, -2.0, 0.0).astype(jnp.bfloat16)
        got = jnp.dot(pool_ref[...], hot, preferred_element_type=jnp.float32)
        feats[t, c] = got.T.astype(jnp.bfloat16)
        lab = -0.5 * jnp.dot(label_rows, hot, preferred_element_type=jnp.float32)
        for k in range(n_c):
            labs[t, k] = lab[0:8, k * share:(k + 1) * share]

    def send_feats(t):
        mine = feats.at[t, c]
        direct = []
        for q in range(1, ny):
            direct.append(send(mine, mine, feat_sem.at[t, q], "centre", lax.rem(c + 2 * q, n_c)))
        return [send(mine, mine, feat_sem.at[t, 0], "centre", sib)], direct

    def forward_feats(t, near, direct):
        for q, copy in enumerate(direct, 1):
            copy.wait_recv()
            slot = feats.at[t, lax.rem(c - 2 * q + n_c, n_c)]
            near.append(send(slot, slot, feat_sem.at[t, ny - 1 + q], "centre", sib))
        for copy in near:
            copy.wait_recv()

    def send_coefs(t):
        mine = coefb.at[t, s]
        return [
            send(mine, mine, coef_sem.at[t, r], "sample", peer) for r, peer in enumerate(s_peers)
        ]

    pick(0)
    cur[...] = coefs_ref[...]
    coefb[0, s] = coefs_ref[...].astype(jnp.bfloat16)
    pl.semaphore_wait(barrier, n_c - 1 + n_s - 1)
    moves = [send_feats(0)]
    coef_moves = send_coefs(0)
    pick(1)
    moves.append(send_feats(1))

    load.wait()

    def square(j, _):
        cols = pl.ds(pl.multiple_of(j * tile, tile), tile)
        block = cen[:, cols].astype(jnp.float32)
        csq[:, cols] = jnp.sum(block * block, axis=0, keepdims=True)
        return 0

    lax.fori_loop(0, cen_dev // tile, square, 0)

    bend = (1.0 / (LENGTH_SCALE * math.log(2.0))) ** 2

    def laplace(t):
        parts = [feats[t, k] for k in range(n_c)]
        ssq = sum(
            jnp.sum(jnp.square(p.astype(jnp.float32)), axis=1, keepdims=True) for p in parts
        ) * 0.25
        if fd % 128 == 0:
            parts = [jnp.concatenate(parts, axis=1)]
        deep = width // len(parts)

        def body(j, _):
            cols = pl.ds(pl.multiple_of(j * tile, tile), tile)
            cross = sum(
                jnp.dot(p, cen[k * deep:(k + 1) * deep, cols], preferred_element_type=jnp.float32)
                for k, p in enumerate(parts)
            )
            arg = ((ssq + csq[:, cols]) + cross) * (bend / width) + bend * EPS
            arg = jnp.maximum(arg, 1e-30)
            value = jnp.exp2(-(arg * lax.rsqrt(arg)))
            for k in range(pieces):
                kern[t, j * pieces + k] = value[:, k * own:(k + 1) * own].astype(jnp.bfloat16)
            return 0

        lax.fori_loop(0, cen_dev // tile, body, 0)

    def residual(t):
        part = sum(
            lax.dot_general(coefb[t, j], kern[t, j], NT, preferred_element_type=jnp.float32)
            for j in range(n_s)
        )
        for k in range(n_c):
            lsend[t, k] = part[:, k * share:(k + 1) * share].astype(LOGIT_WIRE)
        copies = [
            send(lsend.at[t, peer], lrecv.at[t, r], log_sem.at[t, r], "centre", peer)
            for r, peer in enumerate(c_peers)
        ]
        if t + 1 < steps:
            forward_feats(t + 1, *moves[t + 1])
        total = lsend[t, c].astype(jnp.float32)
        for r, copy in enumerate(copies):
            copy.wait_recv()
            total = total + lrecv[t, r].astype(jnp.float32)
        logits = total * logit_scale
        expo = jnp.exp(logits - jnp.max(logits, axis=0, keepdims=True))
        probs = expo / jnp.sum(expo, axis=0, keepdims=True)
        ids = lax.broadcasted_iota(jnp.int32, (classes, share), 0).astype(jnp.float32)
        hot = jnp.where(ids == labs[t, c][0:1, :], 1.0, 0.0)
        resid[t, c] = (probs - hot).astype(jnp.bfloat16)
        mine = resid.at[t, c]
        copies = [
            send(mine, mine, res_sem.at[t, r], "centre", peer) for r, peer in enumerate(c_peers)
        ]
        for copy in copies:
            copy.wait_recv()

    def gradient(t):
        if share % 128 == 0:
            whole = jnp.concatenate([resid[t, k] for k in range(n_c)], axis=1)

            def grad(j):
                return jnp.dot(whole, kern[t, j], preferred_element_type=jnp.float32)
        else:
            def grad(j):
                return sum(
                    jnp.dot(resid[t, k], kern[t, j, k * share:(k + 1) * share, :],
                            preferred_element_type=jnp.float32)
                    for k in range(n_c)
                )
        copies = []
        for r, peer in enumerate(s_peers):
            gsend[t, r] = grad(peer).astype(GRAD_WIRE)
            copies.append(send(gsend.at[t, r], grecv.at[t, r], grad_sem.at[t, r], "sample", peer))
        return grad(s), copies

    forward_feats(0, *moves[0])
    laplace(0)
    for t in range(steps):
        for copy in coef_moves:
            copy.wait_recv()
        residual(t)
        total, copies = gradient(t)
        if t + 1 < steps:
            laplace(t + 1)
        for r, copy in enumerate(copies):
            copy.wait_recv()
            total = total + grecv[t, r].astype(jnp.float32)
        fresh = cur[...] - rate * total
        if t + 1 < steps:
            cur[...] = fresh
            coefb[t + 1, s] = fresh.astype(jnp.bfloat16)
            coef_moves = send_coefs(t + 1)
        else:
            out_ref[...] = fresh
    for copy in started:
        copy.wait_send()


def on_device(n_c, n_s, centres, pool, labels, picks, coefs):
    width, cen_dev = centres.shape
    fd, pool_dev = pool.shape
    steps, batch = picks.shape
    classes, own = coefs.shape
    share = batch // n_c
    bf16, f32 = jnp.bfloat16, jnp.float32
    body = functools.partial(
        kernel, n_c, n_s, LOGIT_GAIN / (cen_dev * n_c), STEP_GAIN * LOGIT_GAIN / (batch * n_s)
    )
    vmem = pl.BlockSpec(memory_space=pltpu.VMEM)
    return pl.pallas_call(
        body,
        out_shape=jax.ShapeDtypeStruct((classes, own), f32),
        in_specs=[pl.BlockSpec(memory_space=pl.ANY)] + [vmem] * 4,
        out_specs=vmem,
        scratch_shapes=[
            pltpu.VMEM((width, cen_dev), bf16),
            pltpu.VMEM((1, cen_dev), f32),
            pltpu.VMEM((steps, n_c, batch, fd), bf16),
            pltpu.VMEM((steps, n_s, batch, own), bf16),
            pltpu.VMEM((steps, n_c, 8, share), f32),
            pltpu.VMEM((steps, n_s, classes, own), bf16),
            pltpu.VMEM((steps, n_c, classes, share), LOGIT_WIRE),
            pltpu.VMEM((steps, n_c - 1, classes, share), LOGIT_WIRE),
            pltpu.VMEM((steps, n_c, classes, share), bf16),
            pltpu.VMEM((steps, n_s - 1, classes, own), GRAD_WIRE),
            pltpu.VMEM((steps, n_s - 1, classes, own), GRAD_WIRE),
            pltpu.VMEM((classes, own), f32),
            pltpu.SemaphoreType.DMA,
            pltpu.SemaphoreType.DMA((steps * (3 * (n_c - 1) + 2 * (n_s - 1)),)),
            pltpu.SemaphoreType.DMA((steps, n_c - 1)),
            pltpu.SemaphoreType.DMA((steps, n_c - 1)),
            pltpu.SemaphoreType.DMA((steps, n_c - 1)),
            pltpu.SemaphoreType.DMA((steps, n_s - 1)),
            pltpu.SemaphoreType.DMA((steps, n_s - 1)),
        ],
        compiler_params=pltpu.CompilerParams(
            collective_id=0, has_side_effects=True, vmem_limit_bytes=60 * 1024 * 1024
        ),
    )(centres, pool, labels.reshape(1, pool_dev), picks, coefs)


def solution(mesh):
    placed = (
        P(None, "centre"),
        P("centre", "sample"),
        P("sample"),
        P(None, "sample"),
        P(None, ("centre", "sample")),
    )
    return jax.shard_map(
        functools.partial(on_device, mesh.shape["centre"], mesh.shape["sample"]),
        mesh=mesh,
        in_specs=placed,
        out_specs=P(None, ("centre", "sample")),
        check_vma=False,
    )
```
